32 devices in a mesh: groups: 2 (over y), blk: 16 (over z, x, core).
Axes of the slice: x: 2, y: 2, z: 4, core: 2. Of those that a mesh axis runs over, the one named last changes fastest.
Arguments:
- queries: bfloat16 [8192, 2560], P(('groups', 'blk')), parts along dimension 0
- keys: bfloat16 [8192, 2560], P(('groups', 'blk')), parts along dimension 0
- values: bfloat16 [8192, 2560], P(('groups', 'blk')), parts along dimension 0
- out_weight: bfloat16 [64, 2560], replicated, may hold values from -0.125 to 0.125
- latent: float32 [64, 8192], P(None, ('groups', 'blk')), parts along dimension 1, may hold values from -6 to 6
- valid: int32 [32], P('groups'), parts along dimension 0, may hold values from 64 to 256, as said below
- timestep: int32 [2], P('groups'), parts along dimension 0, may hold values from 0 to 9
Outputs:
- velocity: float32 [64, 8192], P(None, ('groups', 'blk')), parts along dimension 1
- latent_next: float32 [64, 8192], P(None, ('groups', 'blk')), parts along dimension 1
The draws below stay inside these ranges and needn't reach their ends.
There are 2 independent parts, one for each index of `groups`. The reference program is written for one: setup_inputs(seed, part) draws one part's arguments, and reference() takes and returns one part's arrays. A program takes and returns all parts, laid end to end along the dimension named above; an argument that names none is the same for every part. Nothing has to cross between parts.
Inputs may be any that keep to these rules, and one draw needn't show every extreme that they name: `valid`: blocks whose index is one less than a multiple of 4 hold between 64 and 256 used tokens; all other blocks are full.
All inputs are finite; a program needn't handle non-finite values.
Results may differ from the reference program's by a relative error of at most 0.0065.
Values may be sent and summed in bfloat16 or wider, within the bound.
A program may use at most 128 MiB of HBM per device.

```python
import jax
import jax.numpy as jnp
from jax import lax

HEADS = 20
HEAD_DIM = 128
LATENT_CH = 64
TOK_DEV = 256
R_WIN = 2
FRAME_BLOCKS = 4
STEPS = 10
BLOCKS = 16
TOKENS = 4096
FEATURES = 2560


def draw_queries(key, part):
    base = jax.random.normal(jax.random.fold_in(key, 3), (TOKENS, HEADS * HEAD_DIM), jnp.float32)
    return base.astype(jnp.bfloat16)


def draw_keys(key, part):
    base = jax.random.normal(jax.random.fold_in(key, 5), (TOKENS, HEADS * HEAD_DIM), jnp.float32)
    return base.astype(jnp.bfloat16)


def draw_values(key, part):
    position = jnp.arange(TOKENS, dtype=jnp.float32)[:, None] / TOKENS
    entries = jax.random.normal(jax.random.fold_in(key, 7), (TOKENS, HEADS * HEAD_DIM), jnp.float32)
    base = entries * (0.6 + 1.4 * position)
    return jnp.clip(base, -8.0, 8.0).astype(jnp.bfloat16)


def draw_valid(key, part):
    counts = jax.random.randint(jax.random.fold_in(key, 11), (BLOCKS,), TOK_DEV // 4, TOK_DEV + 1, jnp.int32)
    ending = jnp.arange(BLOCKS, dtype=jnp.int32) % FRAME_BLOCKS == FRAME_BLOCKS - 1
    return jnp.where(ending, counts, jnp.int32(TOK_DEV))


def levels(own_key, dims, pieces, smallest, largest):
    def one(axis_at, parts):
        steps = jax.random.uniform(jax.random.fold_in(jax.random.fold_in(own_key, 6), axis_at), (parts,), jnp.float32, smallest / len(pieces), largest / len(pieces))
        return jnp.repeat(jnp.exp(steps), dims[axis_at] // parts).reshape((-1,) + (1,) * (len(dims) - axis_at - 1))

    factor_of = one(*pieces[0])
    for cut in pieces[1:]:
        factor_of = factor_of * one(*cut)
    return factor_of


def gaussian(own_key, dims, deviation, most, split=(), held_as=jnp.bfloat16):
    values = deviation * jax.random.normal(own_key, dims, jnp.float32)
    if split:
        values = values * levels(own_key, dims, split, -0.22, 0.18)
    return jnp.clip(values, -most, most).astype(held_as)


def setup_inputs(seed: int = 0, part: int = 0) -> dict:
    key_list = jax.random.split(jax.random.key(seed), 8)
    own_keys = jax.random.split(jax.random.fold_in(key_list[7], part), 8)
    return {
        "queries": draw_queries(jax.random.fold_in(jax.random.fold_in(key_list[7], part), 71), part),
        "keys": draw_keys(jax.random.fold_in(jax.random.fold_in(key_list[7], part), 71), part),
        "values": draw_values(jax.random.fold_in(jax.random.fold_in(key_list[7], part), 71), part),
        "out_weight": gaussian(key_list[3], (LATENT_CH, FEATURES), FEATURES ** -0.5, 0.125),
        "latent": gaussian(own_keys[4], (LATENT_CH, TOKENS), 1.0, 6.0, ((1, 16),), jnp.float32),
        "valid": draw_valid(jax.random.fold_in(jax.random.fold_in(key_list[7], part), 71), part),
        "timestep": jax.random.randint(own_keys[6], (1,), 0, STEPS).astype(jnp.int32),
    }


def reference(queries, keys, values, out_weight, latent, valid, timestep):
    span = (2 * R_WIN + 1) * TOK_DEV
    zero_rows = jnp.zeros((R_WIN * TOK_DEV, HEADS * HEAD_DIM), jnp.bfloat16)
    keys_padded = jnp.concatenate([zero_rows, keys, zero_rows], axis=0)
    values_padded = jnp.concatenate([zero_rows, values, zero_rows], axis=0)
    zero_counts = jnp.zeros((R_WIN,), jnp.int32)
    valid_padded = jnp.concatenate([zero_counts, valid.astype(jnp.int32), zero_counts], axis=0)
    slots = jnp.arange(TOK_DEV, dtype=jnp.int32)
    score_scale = 1.0 / jnp.sqrt(jnp.float32(HEAD_DIM))

    def one_block(block):
        start = (block * TOK_DEV).astype(jnp.int32)
        query_heads = lax.dynamic_slice_in_dim(queries, start, TOK_DEV, 0).reshape(TOK_DEV, HEADS, HEAD_DIM).astype(jnp.float32)
        key_heads = lax.dynamic_slice_in_dim(keys_padded, start, span, 0).reshape(span, HEADS, HEAD_DIM).astype(jnp.float32)
        value_heads = lax.dynamic_slice_in_dim(values_padded, start, span, 0).reshape(span, HEADS, HEAD_DIM).astype(jnp.float32)
        counts = lax.dynamic_slice_in_dim(valid_padded, block.astype(jnp.int32), 2 * R_WIN + 1, 0)
        key_used = (slots[None, :] < counts[:, None]).reshape(span)
        scores = jnp.einsum('qhd,khd->hqk', query_heads, key_heads) * score_scale
        scores = jnp.where(key_used[None, None, :], scores, jnp.float32(-1e+30))
        top = lax.optimization_barrier(jnp.max(scores, axis=-1, keepdims=True))
        weights = jnp.exp(scores - top)
        total = lax.optimization_barrier(jnp.sum(weights, axis=-1))
        rounded = weights.astype(jnp.bfloat16).astype(jnp.float32)
        mixed = jnp.einsum('hqk,khd->hqd', rounded, value_heads) / total[:, :, None]
        mixed = jnp.transpose(mixed, (1, 0, 2)).reshape(TOK_DEV, HEADS * HEAD_DIM)
        used = slots < valid[block]
        attn = jnp.where(used[:, None], mixed, 0.0).astype(jnp.bfloat16)
        return lax.dot_general(out_weight, attn, (((1,), (1,)), ((), ())), preferred_element_type=jnp.float32)
    blocks_vel = lax.map(one_block, jnp.arange(BLOCKS, dtype=jnp.int32))
    vel = jnp.transpose(blocks_vel, (1, 0, 2)).reshape(LATENT_CH, TOKENS)
    squares = jnp.sum(vel * vel)
    count = jnp.float32(LATENT_CH) * jnp.sum(valid.astype(jnp.float32))
    rms = jnp.sqrt(squares / count + 1e-06)
    velocity = vel / rms
    level = timestep[0].astype(jnp.float32)
    early = 1.0 - level / STEPS
    later = 1.0 - (level + 1.0) / STEPS
    sigma_early = 5.0 * early / (1.0 + 4.0 * early)
    sigma_later = 5.0 * later / (1.0 + 4.0 * later)
    latent_next = latent + (sigma_later - sigma_early) * velocity
    return (velocity, latent_next)
```

```python
import functools

import jax
import jax.numpy as jnp
from jax import lax
from jax.experimental import pallas as pl
from jax.experimental.pallas import tpu as pltpu
from jax.sharding import PartitionSpec as P

HEAD_DIM = 128
R_WIN = 2
STEPS = 10
UNIT = 4
BF16, F32 = jnp.bfloat16, jnp.float32
NT = (((1,), (1,)), ((), ()))
LOG2E = 1.4426950408889634


def kernel(n, q_hbm, k_hbm, v_hbm, w_ref, valid_ref, vel_ref, sq_ref,
           v_buf, vw_own, qbuf, kbuf, vwbuf, s_buf, vel_acc, vel_in, sq_in,
           loc_sem, v_sem, xs_sem, xr_sem, zs_sem, zr_sem, vs_sem, vr_sem, ss_sem, sr_sem):
    rows = q_hbm.shape[0]
    heads = q_hbm.shape[1] // HEAD_DIM
    mine = heads // UNIT
    units = n // UNIT
    me = lax.axis_index("blk")
    unit = me // UNIT
    slot = me % UNIT
    chip, core = slot // 2, slot % 2
    partner = [slot, 2 * chip + 1 - core, 2 * (1 - chip) + core, 2 * (1 - chip) + 1 - core]

    barrier = pltpu.get_barrier_semaphore()

    @pl.loop(1, n)
    def _(d):
        pl.semaphore_signal(barrier, inc=1, device_id={"blk": (me + d) % n},
                            device_id_type=pl.DeviceIdType.MESH)

    v_copy = pltpu.make_async_copy(v_hbm, v_buf, v_sem)
    v_copy.start()

    def columns(t, j):
        return pl.ds(pl.multiple_of((t * mine + j) * HEAD_DIM, HEAD_DIM), HEAD_DIM)

    def local(j, kind):
        if kind == 0:
            return pltpu.make_async_copy(
                k_hbm.at[:, columns(slot, j)], kbuf.at[j, R_WIN + slot], loc_sem.at[0, j])
        if kind == 1:
            return pltpu.make_async_copy(
                vw_own.at[slot * mine + j], vwbuf.at[j, R_WIN + slot], loc_sem.at[1, j])
        return pltpu.make_async_copy(
            q_hbm.at[:, columns(slot, j)], qbuf.at[j, slot], loc_sem.at[2, j])

    def cross(d, j, kind):
        t = partner[d]
        if kind == 0:
            src, dst = k_hbm.at[:, columns(t, j)], kbuf.at[j, R_WIN + slot]
        elif kind == 1:
            src, dst = vw_own.at[t * mine + j], vwbuf.at[j, R_WIN + slot]
        else:
            src, dst = q_hbm.at[:, columns(t, j)], qbuf.at[j, slot]
        return pltpu.make_async_remote_copy(
            src_ref=src, dst_ref=dst, send_sem=xs_sem.at[d - 1, kind, j],
            recv_sem=xr_sem.at[d - 1, kind, j], device_id={"blk": unit * UNIT + t},
            device_id_type=pl.DeviceIdType.MESH)

    def along(up, j, kind):
        buf = kbuf if kind == 0 else vwbuf
        frm, to = (UNIT, 0) if up else (R_WIN, R_WIN + UNIT)
        return pltpu.make_async_remote_copy(
            src_ref=buf.at[j, pl.ds(frm, R_WIN)], dst_ref=buf.at[j, pl.ds(to, R_WIN)],
            send_sem=zs_sem.at[int(up), kind, j], recv_sem=zr_sem.at[int(up), kind, j],
            device_id={"blk": (me + (UNIT if up else n - UNIT)) % n},
            device_id_type=pl.DeviceIdType.MESH)

    @pl.loop(0, mine)
    def _(j):
        local(j, 0).start()
        local(j, 2).start()

    @pl.when(unit == 0)
    def _():
        kbuf[:, 0:R_WIN] = jnp.zeros((mine, R_WIN, rows, HEAD_DIM), BF16)
        vwbuf[:, 0:R_WIN] = jnp.zeros((mine, R_WIN) + vwbuf.shape[2:], BF16)

    @pl.when(unit == units - 1)
    def _():
        kbuf[:, R_WIN + UNIT:] = jnp.zeros((mine, R_WIN, rows, HEAD_DIM), BF16)
        vwbuf[:, R_WIN + UNIT:] = jnp.zeros((mine, R_WIN) + vwbuf.shape[2:], BF16)

    vel_acc[...] = jnp.zeros_like(vel_acc)
    v_copy.wait()
    for h in range(heads):
        cols = slice(h * HEAD_DIM, (h + 1) * HEAD_DIM)
        vw_own[h] = lax.dot_general(
            w_ref[:, cols], v_buf[:, cols], NT, preferred_element_type=F32).astype(BF16)

    pl.semaphore_wait(barrier, n - 1)

    @pl.loop(0, mine + 1)
    def _(j):
        @pl.when(j < mine)
        def _():
            for kind in (0, 1):
                for d in (2, 3, 1):
                    cross(d, j, kind).start()
            local(j, 1).start()

        @pl.when(j > 0)
        def _():
            for d in (2, 3, 1):
                cross(d, j - 1, 2).start()

    limits = []
    for kb in range(UNIT + 2 * R_WIN):
        block = unit * UNIT - R_WIN + kb
        filled = valid_ref[jnp.clip(block, 0, n - 1)]
        limits.append(jnp.where((block >= 0) & (block < n), filled, 0))
    factor = LOG2E / (HEAD_DIM ** 0.5)
    masked = (0, 1, R_WIN + UNIT - 1, R_WIN + UNIT, R_WIN + UNIT + 1)

    def attend(j):
        row_id = lax.broadcasted_iota(jnp.int32, (rows, rows), 0)
        for qs in range(UNIT):
            queries = qbuf[j, qs]
            top = None
            for kk in range(2 * R_WIN + 1):
                kb = qs + kk
                s = lax.dot_general(kbuf[j, kb], queries, NT, preferred_element_type=F32)
                if kb in masked:
                    s = jnp.where(row_id < limits[kb], s, F32(-1e30))
                s_buf[qs % 2, kk] = s
                part = jnp.max(s, axis=0, keepdims=True)
                top = part if top is None else jnp.maximum(top, part)
            total = None
            out = None
            for kk in range(2 * R_WIN + 1):
                e = jnp.exp2((s_buf[qs % 2, kk] - top) * factor)
                part = jnp.sum(e, axis=0, keepdims=True)
                total = part if total is None else total + part
                o = jnp.dot(vwbuf[j, qs + kk], e.astype(BF16), preferred_element_type=F32)
                out = o if out is None else out + o
            vel_acc[qs] += out / total

    @pl.loop(0, mine + 1)
    def _(j):
        @pl.when(j < mine)
        def _():
            for kind in (0, 1):
                local(j, kind).wait()
                for d in (1, 2, 3):
                    cross(d, j, kind).wait_recv()

            @pl.when(unit < units - 1)
            def _():
                along(True, j, 0).start()
                along(True, j, 1).start()

            @pl.when(unit > 0)
            def _():
                along(False, j, 0).start()
                along(False, j, 1).start()

        @pl.when(j > 0)
        def _():
            i = j - 1
            local(i, 2).wait()
            for d in (1, 2, 3):
                cross(d, i, 2).wait_recv()

            @pl.when(unit > 0)
            def _():
                along(True, i, 0).wait_recv()
                along(True, i, 1).wait_recv()

            @pl.when(unit < units - 1)
            def _():
                along(False, i, 0).wait_recv()
                along(False, i, 1).wait_recv()

            attend(i)

    def give(d):
        return pltpu.make_async_remote_copy(
            src_ref=vel_acc.at[partner[d]], dst_ref=vel_in.at[d - 1],
            send_sem=vs_sem.at[d - 1], recv_sem=vr_sem.at[d - 1],
            device_id={"blk": unit * UNIT + partner[d]},
            device_id_type=pl.DeviceIdType.MESH)

    for d in (2, 3, 1):
        give(d).start()
    vel = vel_acc[slot]
    for d in (1, 2, 3):
        give(d).wait_recv()
        vel = vel + vel_in[d - 1]
    col_id = lax.broadcasted_iota(jnp.int32, vel.shape, 1)
    vel = jnp.where(col_id < valid_ref[me], vel, F32(0))
    vel_ref[...] = vel
    sq_in[0] = jnp.sum((vel * vel).reshape(vel.shape[0] // 8, 8, vel.shape[1]), axis=0)

    def tell(d):
        return pltpu.make_async_remote_copy(
            src_ref=sq_in.at[0], dst_ref=sq_in.at[d],
            send_sem=ss_sem.at[d], recv_sem=sr_sem.at[d],
            device_id={"blk": (me + d) % n}, device_id_type=pl.DeviceIdType.MESH)

    @pl.loop(1, n)
    def _(d):
        tell(d).start()

    @pl.loop(0, mine)
    def _(j):
        for d in (1, 2, 3):
            for kind in (0, 1, 2):
                cross(d, j, kind).wait_send()

        @pl.when(unit < units - 1)
        def _():
            along(True, j, 0).wait_send()
            along(True, j, 1).wait_send()

        @pl.when(unit > 0)
        def _():
            along(False, j, 0).wait_send()
            along(False, j, 1).wait_send()

    for d in (1, 2, 3):
        give(d).wait_send()

    @pl.loop(1, n)
    def _(d):
        tell(d).wait()

    sq_ref[...] = jnp.sum(sq_in[...], axis=0)


def local(n, queries, keys, values, out_weight, latent, valid, timestep):
    rows, features = queries.shape
    channels = out_weight.shape[0]
    heads = features // HEAD_DIM
    mine = heads // UNIT
    held = UNIT + 2 * R_WIN
    hbm = pl.BlockSpec(memory_space=pl.ANY)
    vmem = pl.BlockSpec(memory_space=pltpu.VMEM)
    dma = pltpu.SemaphoreType.DMA
    vel, squares = pl.pallas_call(
        functools.partial(kernel, n),
        out_shape=(jax.ShapeDtypeStruct((channels, rows), F32),
                   jax.ShapeDtypeStruct((8, rows), F32)),
        in_specs=[hbm, hbm, hbm, vmem, pl.BlockSpec(memory_space=pltpu.SMEM)],
        out_specs=(vmem, vmem),
        scratch_shapes=[
            pltpu.VMEM((rows, features), BF16),
            pltpu.VMEM((heads, channels, rows), BF16),
            pltpu.VMEM((mine, UNIT, rows, HEAD_DIM), BF16),
            pltpu.VMEM((mine, held, rows, HEAD_DIM), BF16),
            pltpu.VMEM((mine, held, channels, rows), BF16),
            pltpu.VMEM((2, 2 * R_WIN + 1, rows, rows), F32),
            pltpu.VMEM((UNIT, channels, rows), F32),
            pltpu.VMEM((UNIT - 1, channels, rows), F32),
            pltpu.VMEM((n, 8, rows), F32),
            dma((3, mine)),
            dma,
            dma((UNIT - 1, 3, mine)),
            dma((UNIT - 1, 3, mine)),
            dma((2, 2, mine)),
            dma((2, 2, mine)),
            dma((UNIT - 1,)),
            dma((UNIT - 1,)),
            dma((n,)),
            dma((n,)),
        ],
        compiler_params=pltpu.CompilerParams(
            collective_id=0, has_side_effects=True, vmem_limit_bytes=40 * 1024 * 1024),
    )(queries, keys, values, out_weight, valid)
    count = jnp.float32(channels) * jnp.sum(valid.astype(jnp.float32))
    rms = jnp.sqrt(jnp.sum(squares) / count + 1e-06)
    velocity = vel / rms
    level = timestep[0].astype(jnp.float32)
    early = 1.0 - level / STEPS
    later = 1.0 - (level + 1.0) / STEPS
    sigma_early = 5.0 * early / (1.0 + 4.0 * early)
    sigma_later = 5.0 * later / (1.0 + 4.0 * later)
    return (velocity, latent + (sigma_later - sigma_early) * velocity)


def solution(mesh):
    tokens = P(("groups", "blk"), None)
    spread = P(None, ("groups", "blk"))
    return jax.shard_map(
        functools.partial(local, mesh.shape["blk"]), mesh=mesh,
        in_specs=(tokens, tokens, tokens, P(), spread, P("groups"), P("groups")),
        out_specs=(spread, spread), check_vma=False)
```

```python
import functools

import jax
import jax.numpy as jnp
from jax import lax
from jax.experimental import pallas as pl
from jax.experimental.pallas import tpu as pltpu
from jax.sharding import PartitionSpec as P

HEAD_DIM = 128
R_WIN = 2
STEPS = 10
UNIT = 4
BF16, F32 = jnp.bfloat16, jnp.float32
NT = (((1,), (1,)), ((), ()))
LOG2E = 1.4426950408889634


def kernel(n, q_hbm, k_hbm, v_hbm, w_hbm, valid_ref, step_ref, vel_ref, scale_ref, dt_ref,
           v_buf, w_buf, vw_own, qbuf, kbuf, vwbuf, s_buf, vel_acc, vel_out, vel_in, sq_in,
           loc_sem, v_sem, w_sem, xs_sem, xr_sem, zs_sem, zr_sem, vs_sem, vr_sem, ss_sem, sr_sem):
    rows = q_hbm.shape[0]
    heads = q_hbm.shape[1] // HEAD_DIM
    mine = heads // UNIT
    units = n // UNIT
    me = lax.axis_index("blk")
    unit = me // UNIT
    slot = me % UNIT
    chip, core = slot // 2, slot % 2
    partner = [slot, 2 * chip + 1 - core, 2 * (1 - chip) + core, 2 * (1 - chip) + 1 - core]

    barrier = pltpu.get_barrier_semaphore()

    def greet(device):
        pl.semaphore_signal(barrier, inc=1, device_id={"blk": device},
                            device_id_type=pl.DeviceIdType.MESH)

    near = units - 1 <= mine
    if near:
        for d in (1, 2, 3):
            greet(unit * UNIT + partner[d])

        @pl.when(unit < units - 1)
        def _():
            greet(me + UNIT)

        @pl.when(unit > 0)
        def _():
            greet(me - UNIT)
    else:
        @pl.loop(1, n)
        def _(d):
            greet((me + d) % n)

    v_copy = pltpu.make_async_copy(v_hbm, v_buf, v_sem)
    w_copy = pltpu.make_async_copy(w_hbm, w_buf, w_sem)
    w_copy.start()
    v_copy.start()

    def columns(t, j):
        return pl.ds(pl.multiple_of((t * mine + j) * HEAD_DIM, HEAD_DIM), HEAD_DIM)

    def local(j, kind):
        if kind == 0:
            return pltpu.make_async_copy(
                k_hbm.at[:, columns(slot, j)], kbuf.at[j, R_WIN + slot], loc_sem.at[0, j])
        if kind == 1:
            return pltpu.make_async_copy(
                vw_own.at[slot * mine + j], vwbuf.at[j, R_WIN + slot], loc_sem.at[1, j])
        return pltpu.make_async_copy(
            q_hbm.at[:, columns(slot, j)], qbuf.at[j, slot], loc_sem.at[2, j])

    def cross(d, j, kind):
        t = partner[d]
        if kind == 0:
            src, dst = k_hbm.at[:, columns(t, j)], kbuf.at[j, R_WIN + slot]
        elif kind == 1:
            src, dst = vw_own.at[t * mine + j], vwbuf.at[j, R_WIN + slot]
        else:
            src, dst = q_hbm.at[:, columns(t, j)], qbuf.at[j, slot]
        return pltpu.make_async_remote_copy(
            src_ref=src, dst_ref=dst, send_sem=xs_sem.at[d - 1, kind, j],
            recv_sem=xr_sem.at[d - 1, kind, j], device_id={"blk": unit * UNIT + t},
            device_id_type=pl.DeviceIdType.MESH)

    def along(up, j, kind):
        buf = kbuf if kind == 0 else vwbuf
        frm, to = (UNIT, 0) if up else (R_WIN, R_WIN + UNIT)
        return pltpu.make_async_remote_copy(
            src_ref=buf.at[j, pl.ds(frm, R_WIN)], dst_ref=buf.at[j, pl.ds(to, R_WIN)],
            send_sem=zs_sem.at[int(up), kind, j], recv_sem=zr_sem.at[int(up), kind, j],
            device_id={"blk": (me + (UNIT if up else n - UNIT)) % n},
            device_id_type=pl.DeviceIdType.MESH)

    @pl.loop(0, mine)
    def _(j):
        local(j, 0).start()
        local(j, 2).start()

    @pl.when(unit == 0)
    def _():
        kbuf[:, 0:R_WIN] = jnp.zeros((mine, R_WIN, rows, HEAD_DIM), BF16)
        vwbuf[:, 0:R_WIN] = jnp.zeros((mine, R_WIN) + vwbuf.shape[2:], BF16)

    @pl.when(unit == units - 1)
    def _():
        kbuf[:, R_WIN + UNIT:] = jnp.zeros((mine, R_WIN, rows, HEAD_DIM), BF16)
        vwbuf[:, R_WIN + UNIT:] = jnp.zeros((mine, R_WIN) + vwbuf.shape[2:], BF16)

    vel_acc[...] = jnp.zeros_like(vel_acc)
    if near:
        pl.semaphore_wait(barrier, UNIT - 1 + (unit + units - 1) // units
                          + (2 * units - 2 - unit) // units)
    else:
        pl.semaphore_wait(barrier, n - 1)

    def send_all(kind):
        @pl.loop(0, mine)
        def _(j):
            for d in (2, 3, 1):
                cross(d, j, kind).start()

    send_all(0)
    w_copy.wait()
    v_copy.wait()
    for h in range(heads):
        cols = slice(h * HEAD_DIM, (h + 1) * HEAD_DIM)
        vw_own[h] = lax.dot_general(
            w_buf[:, cols], v_buf[:, cols], NT, preferred_element_type=F32).astype(BF16)
    send_all(1)
    send_all(2)

    @pl.loop(0, mine)
    def _(j):
        local(j, 1).start()

    limits = []
    for kb in range(UNIT + 2 * R_WIN):
        block = unit * UNIT - R_WIN + kb
        filled = valid_ref[jnp.clip(block, 0, n - 1)]
        limits.append(jnp.where((block >= 0) & (block < n), filled, 0))
    factor = LOG2E / (HEAD_DIM ** 0.5)
    masked = (0, 1, R_WIN + UNIT - 1, R_WIN + UNIT, R_WIN + UNIT + 1)

    def attend(j, blocks, after=None):
        row_id = lax.broadcasted_iota(jnp.int32, (rows, rows), 0)
        for qs in blocks:
            queries = qbuf[j, qs]
            top = None
            for kk in range(2 * R_WIN + 1):
                kb = qs + kk
                s = lax.dot_general(kbuf[j, kb], queries, NT, preferred_element_type=F32)
                if kb in masked:
                    s = jnp.where(row_id < limits[kb], s, F32(-1e30))
                s_buf[qs % 2, kk] = s
                part = jnp.max(s, axis=0, keepdims=True)
                top = part if top is None else jnp.maximum(top, part)
            total = None
            out = None
            for kk in range(2 * R_WIN + 1):
                e = jnp.exp2((s_buf[qs % 2, kk] - top) * factor)
                part = jnp.sum(e, axis=0, keepdims=True)
                total = part if total is None else total + part
                o = jnp.dot(vwbuf[j, qs + kk], e.astype(BF16), preferred_element_type=F32)
                out = o if out is None else out + o
            vel_acc[qs] += out / total
            if after is not None:
                after(j, qs)

    def arrive(j, kind):
        @pl.when(unit > 0)
        def _():
            along(True, j, kind).wait_recv()

        @pl.when(unit < units - 1)
        def _():
            along(False, j, kind).wait_recv()

    for kind in (0, 1):
        @pl.loop(0, mine)
        def _(j):
            if kind == 1:
                @pl.when(j < 2)
                def _():
                    arrive(mine - 2 + j, 0)

            @pl.when(j >= 2)
            def _():
                arrive(j - 2, kind)

            local(j, kind).wait()
            for d in (1, 2, 3):
                cross(d, j, kind).wait_recv()

            @pl.when(unit < units - 1)
            def _():
                along(True, j, kind).start()

            @pl.when(unit > 0)
            def _():
                along(False, j, kind).start()

    def give(qs, d):
        return pltpu.make_async_remote_copy(
            src_ref=vel_out.at[qs], dst_ref=vel_in.at[d - 1],
            send_sem=vs_sem.at[d - 1], recv_sem=vr_sem.at[d - 1],
            device_id={"blk": unit * UNIT + qs},
            device_id_type=pl.DeviceIdType.MESH)

    def hand_over(j, qs):
        @pl.when(j == mine - 1)
        def _():
            vel_out[qs] = vel_acc[qs].astype(BF16)
            give(qs, 2 + (qs + core) % 2).start()

    for j in (mine - 2, mine - 1):
        arrive(j, 1)

    def own_chip(blocks):
        @pl.loop(0, mine)
        def _(j):
            local(j, 2).wait()
            cross(1, j, 2).wait_recv()
            attend(j, blocks)

    def other_chip(blocks):
        @pl.loop(0, mine)
        def _(j):
            for d in (2, 3):
                cross(d, j, 2).wait_recv()
            attend(j, blocks, hand_over)

    @pl.when(chip == 0)
    def _():
        own_chip((0, 1))
        other_chip((2, 3))

    @pl.when(chip == 1)
    def _():
        own_chip((2, 3))
        other_chip((0, 1))

    vel_out[partner[1]] = vel_acc[partner[1]].astype(BF16)
    give(partner[1], 1).start()
    vel = vel_acc[slot]
    for d in (1, 2, 3):
        give(partner[d], d).wait_recv()
        vel = vel + vel_in[d - 1].astype(F32)
    col_id = lax.broadcasted_iota(jnp.int32, vel.shape, 1)
    vel = jnp.where(col_id < valid_ref[me], vel, F32(0))
    vel_ref[...] = vel
    sq_in[0] = jnp.sum((vel * vel).reshape(vel.shape[0] // 8, 8, vel.shape[1]), axis=0)

    def tell(d):
        return pltpu.make_async_remote_copy(
            src_ref=sq_in.at[0], dst_ref=sq_in.at[d],
            send_sem=ss_sem.at[d], recv_sem=sr_sem.at[d],
            device_id={"blk": (me + d) % n}, device_id_type=pl.DeviceIdType.MESH)

    @pl.loop(1, n)
    def _(d):
        tell(d).start()

    @pl.loop(0, mine)
    def _(j):
        for d in (1, 2, 3):
            for kind in (0, 1, 2):
                cross(d, j, kind).wait_send()

        @pl.when(unit < units - 1)
        def _():
            along(True, j, 0).wait_send()
            along(True, j, 1).wait_send()

        @pl.when(unit > 0)
        def _():
            along(False, j, 0).wait_send()
            along(False, j, 1).wait_send()

    for d in (1, 2, 3):
        give(partner[d], d).wait_send()

    @pl.loop(1, n)
    def _(d):
        tell(d).wait()

    squares = jnp.sum(jnp.sum(sq_in[...], axis=0), keepdims=True)
    used = lax.fori_loop(0, n, lambda b, acc: acc + valid_ref[b], jnp.int32(0))
    wide = vel.shape
    count = jnp.full(wide, used, jnp.int32).astype(F32) * vel.shape[0]
    scale_ref[...] = 1.0 / jnp.sqrt(jnp.broadcast_to(squares, wide) / count + 1e-06)
    level = jnp.full(wide, step_ref[0], jnp.int32).astype(F32)
    early = 1.0 - level / STEPS
    later = 1.0 - (level + 1.0) / STEPS
    sigma_early = 5.0 * early / (1.0 + 4.0 * early)
    sigma_later = 5.0 * later / (1.0 + 4.0 * later)
    dt_ref[...] = sigma_later - sigma_early


def local(n, queries, keys, values, out_weight, latent, valid, timestep):
    rows, features = queries.shape
    channels = out_weight.shape[0]
    heads = features // HEAD_DIM
    mine = heads // UNIT
    held = UNIT + 2 * R_WIN
    hbm = pl.BlockSpec(memory_space=pl.ANY)
    vmem = pl.BlockSpec(memory_space=pltpu.VMEM)
    smem = pl.BlockSpec(memory_space=pltpu.SMEM)
    dma = pltpu.SemaphoreType.DMA
    vel, scale, dt = pl.pallas_call(
        functools.partial(kernel, n),
        out_shape=(jax.ShapeDtypeStruct((channels, rows), F32),) * 3,
        in_specs=[hbm, hbm, hbm, hbm, smem, smem],
        out_specs=(vmem,) * 3,
        scratch_shapes=[
            pltpu.VMEM((rows, features), BF16),
            pltpu.VMEM((channels, features), BF16),
            pltpu.VMEM((heads, channels, rows), BF16),
            pltpu.VMEM((mine, UNIT, rows, HEAD_DIM), BF16),
            pltpu.VMEM((mine, held, rows, HEAD_DIM), BF16),
            pltpu.VMEM((mine, held, channels, rows), BF16),
            pltpu.VMEM((2, 2 * R_WIN + 1, rows, rows), F32),
            pltpu.VMEM((UNIT, channels, rows), F32),
            pltpu.VMEM((UNIT, channels, rows), BF16),
            pltpu.VMEM((UNIT - 1, channels, rows), BF16),
            pltpu.VMEM((n, 8, rows), F32),
            dma((3, mine)),
            dma,
            dma,
            dma((UNIT - 1, 3, mine)),
            dma((UNIT - 1, 3, mine)),
            dma((2, 2, mine)),
            dma((2, 2, mine)),
            dma((UNIT - 1,)),
            dma((UNIT - 1,)),
            dma((n,)),
            dma((n,)),
        ],
        compiler_params=pltpu.CompilerParams(
            collective_id=0, has_side_effects=True, vmem_limit_bytes=67043328),
    )(queries, keys, values, out_weight, valid, timestep)
    velocity = vel * scale
    return (velocity, latent + dt * velocity)


def solution(mesh):
    tokens = P(("groups", "blk"), None)
    spread = P(None, ("groups", "blk"))
    return jax.shard_map(
        functools.partial(local, mesh.shape["blk"]), mesh=mesh,
        in_specs=(tokens, tokens, tokens, P(), spread, P("groups"), P("groups")),
        out_specs=(spread, spread), check_vma=False)
```

```python
import functools

import jax
import jax.numpy as jnp
from jax import lax
from jax.experimental import pallas as pl
from jax.experimental.pallas import tpu as pltpu
from jax.sharding import PartitionSpec as P

HEAD_DIM = 128
R_WIN = 2
STEPS = 10
UNIT = 4
BF16, F32 = jnp.bfloat16, jnp.float32
NT = (((1,), (1,)), ((), ()))
LOG2E = 1.4426950408889634


def kernel(n, q_hbm, k_hbm, v_hbm, w_hbm, valid_ref, step_ref, vel_ref, scale_ref, dt_ref,
           v_buf, w_buf, vw_own, qbuf, kbuf, vwbuf, s_buf, vel_acc, vel_out, vel_in, sq_in,
           loc_sem, v_sem, w_sem, xs_sem, xr_sem, zs_sem, zr_sem, vs_sem, vr_sem, ss_sem, sr_sem):
    rows = q_hbm.shape[0]
    heads = q_hbm.shape[1] // HEAD_DIM
    mine = heads // UNIT
    units = n // UNIT
    me = lax.axis_index("blk")
    unit = me // UNIT
    slot = me % UNIT
    chip, core = slot // 2, slot % 2
    partner = [slot, 2 * chip + 1 - core, 2 * (1 - chip) + core, 2 * (1 - chip) + 1 - core]

    barrier = pltpu.get_barrier_semaphore()

    def greet(device):
        pl.semaphore_signal(barrier, inc=1, device_id={"blk": device},
                            device_id_type=pl.DeviceIdType.MESH)

    near = 2 * (units - 1) <= mine + 1
    if near:
        for d in (1, 2, 3):
            greet(unit * UNIT + partner[d])

        @pl.when(unit < units - 1)
        def _():
            greet(me + UNIT)

        @pl.when(unit > 0)
        def _():
            greet(me - UNIT)
    else:
        @pl.loop(1, n)
        def _(d):
            greet((me + d) % n)

    v_copy = pltpu.make_async_copy(v_hbm, v_buf, v_sem)
    w_copy = pltpu.make_async_copy(w_hbm, w_buf, w_sem)
    w_copy.start()
    v_copy.start()

    def columns(t, j):
        return pl.ds(pl.multiple_of((t * mine + j) * HEAD_DIM, HEAD_DIM), HEAD_DIM)

    def local(j, kind):
        if kind == 0:
            return pltpu.make_async_copy(
                k_hbm.at[:, columns(slot, j)], kbuf.at[j, R_WIN + slot], loc_sem.at[0, j])
        if kind == 1:
            return pltpu.make_async_copy(
                vw_own.at[slot * mine + j], vwbuf.at[j, R_WIN + slot], loc_sem.at[1, j])
        return pltpu.make_async_copy(
            q_hbm.at[:, columns(slot, j)], qbuf.at[j, slot], loc_sem.at[2, j])

    def cross(d, j, kind):
        t = partner[d]
        if kind == 0:
            src, dst = k_hbm.at[:, columns(t, j)], kbuf.at[j, R_WIN + slot]
        elif kind == 1:
            src, dst = vw_own.at[t * mine + j], vwbuf.at[j, R_WIN + slot]
        else:
            src, dst = q_hbm.at[:, columns(t, j)], qbuf.at[j, slot]
        return pltpu.make_async_remote_copy(
            src_ref=src, dst_ref=dst, send_sem=xs_sem.at[d - 1, kind, j],
            recv_sem=xr_sem.at[d - 1, kind, j], device_id={"blk": unit * UNIT + t},
            device_id_type=pl.DeviceIdType.MESH)

    def along(up, j, kind):
        buf = kbuf if kind == 0 else vwbuf
        frm, to = (UNIT, 0) if up else (R_WIN, R_WIN + UNIT)
        return pltpu.make_async_remote_copy(
            src_ref=buf.at[j, pl.ds(frm, R_WIN)], dst_ref=buf.at[j, pl.ds(to, R_WIN)],
            send_sem=zs_sem.at[int(up), kind, j], recv_sem=zr_sem.at[int(up), kind, j],
            device_id={"blk": (me + (UNIT if up else n - UNIT)) % n},
            device_id_type=pl.DeviceIdType.MESH)

    @pl.loop(0, mine)
    def _(j):
        local(j, 0).start()
        local(j, 2).start()

    @pl.when(unit == 0)
    def _():
        kbuf[:, 0:R_WIN] = jnp.zeros((mine, R_WIN, rows, HEAD_DIM), BF16)
        vwbuf[:, 0:R_WIN] = jnp.zeros((mine, R_WIN) + vwbuf.shape[2:], BF16)

    @pl.when(unit == units - 1)
    def _():
        kbuf[:, R_WIN + UNIT:] = jnp.zeros((mine, R_WIN, rows, HEAD_DIM), BF16)
        vwbuf[:, R_WIN + UNIT:] = jnp.zeros((mine, R_WIN) + vwbuf.shape[2:], BF16)

    vel_acc[...] = jnp.zeros_like(vel_acc)
    if near:
        pl.semaphore_wait(barrier, UNIT - 1 + (unit + units - 1) // units
                          + (2 * units - 2 - unit) // units)
    else:
        pl.semaphore_wait(barrier, n - 1)

    def send(j, kind):
        for d in (2, 3, 1):
            cross(d, j, kind).start()

    early = min(2, mine)
    for j in range(early):
        send(j, 0)

    @pl.loop(0, mine)
    def _(j):
        cross(1, j, 2).start()

    w_copy.wait()
    v_copy.wait()
    for h in range(heads):
        cols = slice(h * HEAD_DIM, (h + 1) * HEAD_DIM)
        vw_own[h] = lax.dot_general(
            w_buf[:, cols], v_buf[:, cols], NT, preferred_element_type=F32).astype(BF16)

    @pl.loop(0, mine)
    def _(j):
        local(j, 1).start()
        send(j, 1)

        @pl.when(j + early < mine)
        def _():
            send(j + early, 0)

    @pl.loop(0, mine)
    def _(j):
        for d in (2, 3):
            cross(d, j, 2).start()

    limits = []
    for kb in range(UNIT + 2 * R_WIN):
        block = unit * UNIT - R_WIN + kb
        filled = valid_ref[jnp.clip(block, 0, n - 1)]
        limits.append(jnp.where((block >= 0) & (block < n), filled, 0))
    factor = LOG2E / (HEAD_DIM ** 0.5)
    masked = (0, 1, R_WIN + UNIT - 1, R_WIN + UNIT, R_WIN + UNIT + 1)

    def attend(j, blocks, after=None):
        row_id = lax.broadcasted_iota(jnp.int32, (rows, rows), 0)
        for qs in blocks:
            queries = qbuf[j, qs]
            top = None
            for kk in range(2 * R_WIN + 1):
                kb = qs + kk
                s = lax.dot_general(kbuf[j, kb], queries, NT, preferred_element_type=F32)
                if kb in masked:
                    s = jnp.where(row_id < limits[kb], s, F32(-1e30))
                s_buf[qs % 2, kk] = s
                part = jnp.max(s, axis=0, keepdims=True)
                top = part if top is None else jnp.maximum(top, part)
            total = None
            out = None
            for kk in range(2 * R_WIN + 1):
                e = jnp.exp2((s_buf[qs % 2, kk] - top) * factor)
                part = jnp.sum(e, axis=0, keepdims=True)
                total = part if total is None else total + part
                o = jnp.dot(vwbuf[j, qs + kk], e.astype(BF16), preferred_element_type=F32)
                out = o if out is None else out + o
            vel_acc[qs] += out / total
            if after is not None:
                after(j, qs)

    def arrive(j, kind):
        @pl.when(unit > 0)
        def _():
            along(True, j, kind).wait_recv()

        @pl.when(unit < units - 1)
        def _():
            along(False, j, kind).wait_recv()

    def gather(j):
        for kind in (0, 1):
            local(j, kind).wait()
            for d in (1, 2, 3):
                cross(d, j, kind).wait_recv()

            @pl.when(unit < units - 1)
            def _():
                along(True, j, kind).start()

            @pl.when(unit > 0)
            def _():
                along(False, j, kind).start()

    def give(qs, d):
        return pltpu.make_async_remote_copy(
            src_ref=vel_out.at[qs], dst_ref=vel_in.at[d - 1],
            send_sem=vs_sem.at[d - 1], recv_sem=vr_sem.at[d - 1],
            device_id={"blk": unit * UNIT + qs},
            device_id_type=pl.DeviceIdType.MESH)

    def hand_over(j, qs):
        @pl.when(j == mine - 1)
        def _():
            vel_out[qs] = vel_acc[qs].astype(BF16)
            give(qs, 2 + (qs + core) % 2).start()

    def own_chip(blocks):
        @pl.loop(0, mine + 1)
        def _(j):
            @pl.when(j < mine)
            def _():
                gather(j)

            @pl.when(j > 0)
            def _():
                i = j - 1
                arrive(i, 0)
                arrive(i, 1)
                local(i, 2).wait()
                cross(1, i, 2).wait_recv()
                attend(i, blocks)

    def other_chip(blocks):
        @pl.loop(0, mine)
        def _(j):
            for d in (2, 3):
                cross(d, j, 2).wait_recv()
            attend(j, blocks, hand_over)

    def on_chip():
        vel_out[partner[1]] = vel_acc[partner[1]].astype(BF16)
        give(partner[1], 1).start()

    @pl.when(chip == 0)
    def _():
        own_chip((0, 1))
        on_chip()
        other_chip((2, 3))

    @pl.when(chip == 1)
    def _():
        own_chip((2, 3))
        on_chip()
        other_chip((0, 1))

    vel = vel_acc[slot]
    for d in (1, 2, 3):
        give(partner[d], d).wait_recv()
        vel = vel + vel_in[d - 1].astype(F32)
    col_id = lax.broadcasted_iota(jnp.int32, vel.shape, 1)
    vel = jnp.where(col_id < valid_ref[me], vel, F32(0))
    vel_ref[...] = vel
    square = jnp.sum(vel * vel, axis=0, keepdims=True)
    lanes = sq_in.shape[2]
    sq_in[0] = sum(square[:, i:i + lanes] for i in range(0, square.shape[1], lanes))

    def tell(d):
        return pltpu.make_async_remote_copy(
            src_ref=sq_in.at[0], dst_ref=sq_in.at[d],
            send_sem=ss_sem.at[d], recv_sem=sr_sem.at[d],
            device_id={"blk": (me + d) % n}, device_id_type=pl.DeviceIdType.MESH)

    @pl.loop(1, n)
    def _(d):
        tell(d).start()

    @pl.loop(0, mine)
    def _(j):
        for d in (1, 2, 3):
            for kind in (0, 1, 2):
                cross(d, j, kind).wait_send()

        @pl.when(unit < units - 1)
        def _():
            along(True, j, 0).wait_send()
            along(True, j, 1).wait_send()

        @pl.when(unit > 0)
        def _():
            along(False, j, 0).wait_send()
            along(False, j, 1).wait_send()

    for d in (1, 2, 3):
        give(partner[d], d).wait_send()

    @pl.loop(1, n)
    def _(d):
        tell(d).wait()

    squares = jnp.sum(jnp.sum(sq_in[...], axis=0), keepdims=True)
    used = lax.fori_loop(0, n, lambda b, acc: acc + valid_ref[b], jnp.int32(0))
    wide = vel.shape
    count = jnp.full(wide, used, jnp.int32).astype(F32) * vel.shape[0]
    scale_ref[...] = 1.0 / jnp.sqrt(jnp.broadcast_to(squares, wide) / count + 1e-06)
    level = jnp.full(wide, step_ref[0], jnp.int32).astype(F32)
    early = 1.0 - level / STEPS
    later = 1.0 - (level + 1.0) / STEPS
    sigma_early = 5.0 * early / (1.0 + 4.0 * early)
    sigma_later = 5.0 * later / (1.0 + 4.0 * later)
    dt_ref[...] = sigma_later - sigma_early


def local(n, queries, keys, values, out_weight, latent, valid, timestep):
    rows, features = queries.shape
    channels = out_weight.shape[0]
    heads = features // HEAD_DIM
    mine = heads // UNIT
    held = UNIT + 2 * R_WIN
    hbm = pl.BlockSpec(memory_space=pl.ANY)
    vmem = pl.BlockSpec(memory_space=pltpu.VMEM)
    smem = pl.BlockSpec(memory_space=pltpu.SMEM)
    dma = pltpu.SemaphoreType.DMA
    vel, scale, dt = pl.pallas_call(
        functools.partial(kernel, n),
        out_shape=(jax.ShapeDtypeStruct((channels, rows), F32),) * 3,
        in_specs=[hbm, hbm, hbm, hbm, smem, smem],
        out_specs=(vmem,) * 3,
        scratch_shapes=[
            pltpu.VMEM((rows, features), BF16),
            pltpu.VMEM((channels, features), BF16),
            pltpu.VMEM((heads, channels, rows), BF16),
            pltpu.VMEM((mine, UNIT, rows, HEAD_DIM), BF16),
            pltpu.VMEM((mine, held, rows, HEAD_DIM), BF16),
            pltpu.VMEM((mine, held, channels, rows), BF16),
            pltpu.VMEM((2, 2 * R_WIN + 1, rows, rows), F32),
            pltpu.VMEM((UNIT, channels, rows), F32),
            pltpu.VMEM((UNIT, channels, rows), BF16),
            pltpu.VMEM((UNIT - 1, channels, rows), BF16),
            pltpu.VMEM((n, 1, HEAD_DIM), F32),
            dma((3, mine)),
            dma,
            dma,
            dma((UNIT - 1, 3, mine)),
            dma((UNIT - 1, 3, mine)),
            dma((2, 2, mine)),
            dma((2, 2, mine)),
            dma((UNIT - 1,)),
            dma((UNIT - 1,)),
            dma((n,)),
            dma((n,)),
        ],
        compiler_params=pltpu.CompilerParams(
            collective_id=0, has_side_effects=True, vmem_limit_bytes=67043328),
    )(queries, keys, values, out_weight, valid, timestep)
    velocity = vel * scale
    return (velocity, latent + dt * velocity)


def solution(mesh):
    tokens = P(("groups", "blk"), None)
    spread = P(None, ("groups", "blk"))
    return jax.shard_map(
        functools.partial(local, mesh.shape["blk"]), mesh=mesh,
        in_specs=(tokens, tokens, tokens, P(), spread, P("groups"), P("groups")),
        out_specs=(spread, spread), check_vma=False)
```
